32 devices in a mesh: grp: 4 (over y, core), dom: 8 (over z, x).
Axes of the slice: x: 2, y: 2, z: 4, core: 2. Of those that a mesh axis runs over, the one named last changes fastest.
Arguments:
- element_state: float32 [56, 9, 20480], P(None, None, ('grp', 'dom')), may hold values from -6 to 6
- stiffness: float32 [3, 56, 56], replicated, may hold values from -0.75 to 0.75
- flux_local: float32 [4, 56, 56], replicated, may hold values from -0.75 to 0.75
- flux_remote: float32 [4, 56, 56], replicated, may hold values from -0.75 to 0.75
- star_matrix: float32 [3, 9, 9, 20480], P(None, None, None, ('grp', 'dom')), may hold values from -0.18 to 0.18
- face_local: float32 [4, 9, 9, 20480], P(None, None, None, ('grp', 'dom')), may hold values from -0.15 to 0.15
- face_remote: float32 [4, 9, 9, 20480], P(None, None, None, ('grp', 'dom')), may hold values from -0.15 to 0.15
- energy_weight: float32 [9, 20480], P(None, ('grp', 'dom')), may hold values from 0.5 to 18
- face_neighbour: int32 [4, 20480], P(None, ('grp', 'dom')), may hold values from 0 to 1151, as said below
- element_count: int32 [32], P(('grp', 'dom')), may hold values from 160 to 640, as said below
- send_count: int32 [32, 8], P(('grp', 'dom')), may hold values from 0 to 64, as said below
- send_element: int32 [32, 8, 64], P(('grp', 'dom')), may hold values from 0 to 639, as said below
- receiver_element: int32 [512], P(('grp', 'dom')), may hold values from 0 to 639, as said below
- receiver_slot: int32 [512], P(('grp', 'dom')), may hold values from 0 to 127, as said below
- receiver_weight: float32 [56, 512], P(None, ('grp', 'dom')), may hold values from -0.75 to 0.75
Outputs:
- new_state: float32 [56, 9, 20480], P(None, None, ('grp', 'dom'))
- energy: float32 [4, 3], P('grp')
- traces: float32 [3, 9, 512], P(None, None, ('grp', 'dom'))
The draws below stay inside these ranges and needn't reach their ends.
Inputs may be any that keep to these rules, and one draw needn't show every extreme that they name: The first element_count[p] slots of a partition are active. In every slab 4 partitions in a row along dom (cyclically) hold 640 active elements; the others hold from 160 to 320. `send_count`: every partition has exactly 64 in one of its first 6 slots. `send_element`: names active elements of the sending partition. `face_neighbour`: values below 640 name active elements of the partition itself. `receiver_element`: names an active element of the owning partition. `receiver_slot`: within each slab a permutation of the 128 rows.
All inputs are finite; a program needn't handle non-finite values.
Results may differ from the reference program's by a relative error of at most 0.0001.
Values sent between devices are 32-bit elements; how exact they have to be, the bound alone decides.
A program may use at most 128 MiB of HBM per device.

```python
import jax
import jax.numpy as jnp
from jax import lax

BASIS_MODES = 56
QUANTITIES = 9
DIMENSIONS = 3
ELEM_FACES = 4
PEER_REACH = 3
TIME_STEPS = 3
HALO_CAP = 64
ELEM_PAD = 640
REC_DEV = 16
GROUPS = 4
GROUP_SIZE = 8
PARTITIONS = 32
PEER_SLOTS = 8
ELEMENTS = 20480
RECEIVERS = 512


def partition_counts(key):
    base = jax.random.fold_in(key, 101)
    lighter = jax.random.randint(jax.random.fold_in(base, 1), (PARTITIONS,), ELEM_PAD // 4, ELEM_PAD // 2 + 1)
    window = jax.random.randint(jax.random.fold_in(base, 2), (GROUPS,), 0, GROUP_SIZE)
    numbers = jnp.arange(PARTITIONS, dtype=jnp.int32)
    position = (numbers % GROUP_SIZE - window[numbers // GROUP_SIZE]) % GROUP_SIZE
    return jnp.where(position < 4, ELEM_PAD, lighter).astype(jnp.int32)


def draw_element_count(key, part):
    return partition_counts(key)


def draw_send_count(key, part):
    counted = jax.random.randint(jax.random.fold_in(key, 201), (PARTITIONS, PEER_SLOTS), 0, HALO_CAP + 1)
    fullest = jax.random.randint(jax.random.fold_in(key, 202), (PARTITIONS, 1), 0, 2 * PEER_REACH)
    slots_row = jnp.arange(PEER_SLOTS, dtype=jnp.int32)[None, :]
    return jnp.where(slots_row == fullest, HALO_CAP, counted).astype(jnp.int32)


def draw_send_element(key, part):
    counts = partition_counts(key)
    return jax.random.randint(jax.random.fold_in(key, 301), (PARTITIONS, PEER_SLOTS, HALO_CAP), 0, counts[:, None, None]).astype(jnp.int32)


def draw_face_neighbour(key, part):
    counts = partition_counts(key)
    limits = jnp.repeat(counts, ELEM_PAD, total_repeat_length=ELEMENTS)[None, :]
    own_side = jax.random.randint(jax.random.fold_in(key, 401), (ELEM_FACES, ELEMENTS), 0, limits)
    far_side = ELEM_PAD + jax.random.randint(jax.random.fold_in(key, 402), (ELEM_FACES, ELEMENTS), 0, PEER_SLOTS * HALO_CAP)
    chosen = jax.random.randint(jax.random.fold_in(key, 403), (ELEM_FACES, ELEMENTS), 0, 4) == 0
    return jnp.where(chosen, far_side, own_side).astype(jnp.int32)


def draw_receiver_element(key, part):
    counts = partition_counts(key)
    limits = jnp.repeat(counts, REC_DEV, total_repeat_length=RECEIVERS)
    return jax.random.randint(jax.random.fold_in(key, 501), (RECEIVERS,), 0, limits).astype(jnp.int32)


def draw_receiver_slot(key, part):
    group_keys = jax.random.split(jax.random.fold_in(key, 601), GROUPS)
    orders = jax.vmap(lambda group_key: jax.random.permutation(group_key, GROUP_SIZE * REC_DEV))(group_keys)
    return orders.reshape(-1).astype(jnp.int32)


def draw_energy_weight(key, part):
    uniform_part = jax.random.uniform(jax.random.fold_in(key, 701), (QUANTITIES, ELEMENTS), jnp.float32)
    position = (jnp.arange(ELEMENTS, dtype=jnp.int32) // ELEM_PAD % GROUP_SIZE).astype(jnp.float32)
    rising = 1.0 + 2.0 * position / (GROUP_SIZE - 1)
    return (jnp.exp(jnp.log(0.5) + uniform_part * jnp.log(4.0)) * rising).astype(jnp.float32)


def level_of(key, shape, cuts, low, largest):
    gain = 1.0
    for axis_at, blocks in cuts:
        draws = jax.random.uniform(jax.random.fold_in(jax.random.fold_in(key, 6), axis_at), (blocks,), jnp.float32, low / len(cuts), largest / len(cuts))
        gain = gain * jnp.repeat(jnp.exp(draws), shape[axis_at] // blocks).reshape((-1,) + (1,) * (len(shape) - 1 - axis_at))
    return gain


def normal_values(rng, shape, deviation, bound, cuts=(), kind=jnp.bfloat16):
    result = deviation * jax.random.normal(rng, shape, jnp.float32)
    if cuts:
        result = result * level_of(rng, shape, cuts, -0.22, 0.18)
    return jnp.clip(result, -bound, bound).astype(kind)


def setup_inputs(seed: int = 0) -> dict:
    arg_keys = jax.random.split(jax.random.key(seed), 16)
    element_state = normal_values(arg_keys[0], (BASIS_MODES, QUANTITIES, ELEMENTS), 1.0, 6.0, ((2, 32),), jnp.float32)
    stiffness = normal_values(arg_keys[1], (DIMENSIONS, BASIS_MODES, BASIS_MODES), BASIS_MODES ** -0.5, 0.75, (), jnp.float32)
    flux_local = normal_values(arg_keys[2], (ELEM_FACES, BASIS_MODES, BASIS_MODES), BASIS_MODES ** -0.5, 0.75, (), jnp.float32)
    flux_remote = normal_values(arg_keys[3], (ELEM_FACES, BASIS_MODES, BASIS_MODES), BASIS_MODES ** -0.5, 0.75, (), jnp.float32)
    star_matrix = normal_values(arg_keys[4], (DIMENSIONS, QUANTITIES, QUANTITIES, ELEMENTS), 0.03, 0.18, ((3, 32),), jnp.float32)
    face_local = normal_values(arg_keys[5], (ELEM_FACES, QUANTITIES, QUANTITIES, ELEMENTS), 0.025, 0.15, ((3, 32),), jnp.float32)
    face_remote = normal_values(arg_keys[6], (ELEM_FACES, QUANTITIES, QUANTITIES, ELEMENTS), 0.025, 0.15, ((3, 32),), jnp.float32)
    energy_weight = draw_energy_weight(jax.random.fold_in(arg_keys[15], 71), 0)
    face_neighbour = draw_face_neighbour(jax.random.fold_in(arg_keys[15], 71), 0)
    element_count = draw_element_count(jax.random.fold_in(arg_keys[15], 71), 0)
    send_count = draw_send_count(jax.random.fold_in(arg_keys[15], 71), 0)
    send_element = draw_send_element(jax.random.fold_in(arg_keys[15], 71), 0)
    receiver_element = draw_receiver_element(jax.random.fold_in(arg_keys[15], 71), 0)
    receiver_slot = draw_receiver_slot(jax.random.fold_in(arg_keys[15], 71), 0)
    receiver_weight = normal_values(arg_keys[14], (BASIS_MODES, RECEIVERS), BASIS_MODES ** -0.5, 0.75, ((1, 32),), jnp.float32)
    return dict(element_state=element_state, stiffness=stiffness, flux_local=flux_local, flux_remote=flux_remote, star_matrix=star_matrix, face_local=face_local, face_remote=face_remote, energy_weight=energy_weight, face_neighbour=face_neighbour, element_count=element_count, send_count=send_count, send_element=send_element, receiver_element=receiver_element, receiver_slot=receiver_slot, receiver_weight=receiver_weight)


highest = lax.Precision.HIGHEST


def modal(matrix, field):
    flat = field.reshape(field.shape[0], -1)
    product = jnp.dot(matrix, flat, precision=highest, preferred_element_type=jnp.float32)
    return product.reshape((matrix.shape[0],) + field.shape[1:])


def quantity_map(matrices, field):
    return jnp.einsum("pqe,bqe->bpe", matrices, field, precision=highest)


def per_partition(array):
    shaped = array.reshape(array.shape[:-1] + (PARTITIONS, ELEM_PAD))
    return jnp.moveaxis(shaped, -2, 0)


def slot_offset(slot_number):
    if slot_number < PEER_REACH:
        return slot_number + 1
    if slot_number < 2 * PEER_REACH:
        return PEER_REACH - 1 - slot_number
    if slot_number == 2 * PEER_REACH:
        return 1
    return -1


def reference(element_state, stiffness, flux_local, flux_remote, star_matrix, face_local, face_remote, energy_weight, face_neighbour, element_count, send_count, send_element, receiver_element, receiver_slot, receiver_weight):
    fields = per_partition(element_state)
    stars = per_partition(star_matrix)
    local_faces = per_partition(face_local)
    remote_faces = per_partition(face_remote)
    weights = per_partition(energy_weight)
    neighbours = per_partition(face_neighbour)
    receiver_rows = jnp.moveaxis(receiver_weight.reshape(BASIS_MODES, PARTITIONS, REC_DEV), 1, 0)
    receiver_cells = receiver_element.reshape(PARTITIONS, REC_DEV)
    numbers = jnp.arange(PARTITIONS, dtype=jnp.int32)
    group_of = numbers // GROUP_SIZE
    place_of = numbers % GROUP_SIZE
    source_list = []
    present_list = []
    for slot_number in range(PEER_SLOTS):
        offset = slot_offset(slot_number)
        if slot_number < 2 * PEER_REACH:
            source_list.append(group_of * GROUP_SIZE + (place_of - offset) % GROUP_SIZE)
            present_list.append(jnp.ones((PARTITIONS,), dtype=bool))
        else:
            other = group_of - offset
            present_list.append((other >= 0) & (other < GROUPS))
            source_list.append(jnp.clip(other, 0, GROUPS - 1) * GROUP_SIZE + place_of)
    sources = jnp.stack(source_list, 1).astype(jnp.int32)
    present = jnp.stack(present_list, 1)
    live_mask = jnp.arange(ELEM_PAD, dtype=jnp.int32)[None, :] < element_count[:, None]
    slot_live = jnp.arange(HALO_CAP, dtype=jnp.int32)[None, None, :] < send_count[:, :, None]
    denominator = GROUP_SIZE * ELEM_PAD * BASIS_MODES * QUANTITIES
    global_slot = ((jnp.arange(RECEIVERS, dtype=jnp.int32) // (GROUP_SIZE * REC_DEV)) * (GROUP_SIZE * REC_DEV) + receiver_slot).astype(jnp.int32)

    def pack(field, elements, live):
        taken = jnp.take(field, elements, axis=2)
        return jnp.where(live[None, None], taken, jnp.float32(0.0))

    def advance(fields):
        messages = jax.vmap(pack)(fields, send_element, slot_live)

        def update_one(items):
            field, star_here, local_here, remote_here, neighbour_here, source_here, present_here, live_here = items
            pieces = []
            for slot_number in range(PEER_SLOTS):
                sent = lax.dynamic_index_in_dim(messages, source_here[slot_number], 0, keepdims=False)[:, :, slot_number, :]
                pieces.append(jnp.where(present_here[slot_number], sent, jnp.float32(0.0)))
            halo = jnp.stack(pieces, 2).reshape(BASIS_MODES, QUANTITIES, PEER_SLOTS * HALO_CAP)
            extended = jnp.concatenate([field, halo], 2)
            change = jnp.zeros(field.shape, jnp.float32)
            for dimension in range(DIMENSIONS):
                change = change + quantity_map(star_here[dimension], modal(stiffness[dimension], field))
            for face_number in range(ELEM_FACES):
                change = change - quantity_map(local_here[face_number], modal(flux_local[face_number], field))
                nearby = jnp.take(extended, neighbour_here[face_number], axis=2)
                change = change - quantity_map(remote_here[face_number], modal(flux_remote[face_number], nearby))
            return jnp.where(live_here[None, None, :], field + change, field)

        return lax.map(update_one, (fields, stars, local_faces, remote_faces, neighbours, sources, present, live_mask))

    energies = []
    tables = []
    for time_step in range(TIME_STEPS):
        fields = advance(fields)
        squares = jnp.sum(fields * fields, axis=1)
        terms = 0.5 * jnp.sum(jnp.where(live_mask[:, None, :], weights * squares, jnp.float32(0.0)), axis=(1, 2))
        energies.append(terms.reshape(GROUPS, GROUP_SIZE).sum(1) / denominator)

        def sample(field, elements, rows_here):
            return jnp.einsum("br,bqr->qr", rows_here, jnp.take(field, elements, axis=2), precision=highest)

        values = jax.vmap(sample)(fields, receiver_cells, receiver_rows)
        flat = jnp.moveaxis(values, 0, 1).reshape(QUANTITIES, RECEIVERS)
        tables.append(jnp.zeros((QUANTITIES, RECEIVERS), jnp.float32).at[:, global_slot].set(flat))
    new_state = jnp.moveaxis(fields, 0, 2).reshape(BASIS_MODES, QUANTITIES, ELEMENTS)
    return new_state, jnp.stack(energies, 1), jnp.stack(tables, 0)
```

```python
import functools

import jax
import jax.numpy as jnp
from jax import lax
from jax.experimental import pallas as pl
from jax.experimental.pallas import tpu as pltpu
from jax.sharding import PartitionSpec as P

PEER_REACH = 3
TIME_STEPS = 3
LANES = 128


def round_up(value, multiple):
    return (value + multiple - 1) // multiple * multiple


def split(value):
    high = value.astype(jnp.bfloat16)
    low = (value - high.astype(jnp.float32)).astype(jnp.bfloat16)
    return high, low


def pad_rows(value, rows):
    if value.shape[0] == rows:
        return value
    fill = jnp.zeros((rows - value.shape[0],) + value.shape[1:], value.dtype)
    return jnp.concatenate([value, fill], 0)


def one_hot(rows, names):
    place = lax.broadcasted_iota(jnp.int32, (rows, names.shape[1]), 0)
    return jnp.where(place == names, 1.0, 0.0).astype(jnp.bfloat16)


def dot(a, b):
    return jnp.dot(a, b, preferred_element_type=jnp.float32)


def stacked_matrix(matrices):
    padded = round_up(matrices.shape[2], 16)
    wide = jnp.pad(matrices, ((0, 0), (0, 0), (0, padded - matrices.shape[2])))
    high = lax.reduce_precision(wide, 8, 7)
    low = (wide - high).astype(jnp.bfloat16)
    high = high.astype(jnp.bfloat16)
    return jnp.concatenate([high, high, low], 2)


def row_chunks(rows):
    middle = min(rows, 32)
    return [(0, middle), (middle, rows)] if middle < rows else [(0, rows)]


def pack_kernel(padded, top, x_ref, names_ref, weight_ref, rec_ref, gains_ref, msg_ref, split_ref, value_ref, energy_ref, taken):
    quantities, basis, elements = x_ref.shape
    width = 2 * LANES
    total = jnp.zeros((1, elements), jnp.float32)
    for q in range(quantities):
        field = x_ref[q]
        total = total + gains_ref[q : q + 1, :] * jnp.sum(field * field, axis=0, keepdims=True)
        high, low = split(pad_rows(field, padded))
        split_ref[2 * q * padded : (2 * q + 1) * padded, :] = high
        split_ref[(2 * q + 1) * padded : (2 * q + 2) * padded, :] = low
    energy_ref[...] = total
    picked = dot(split_ref[...], one_hot(elements, rec_ref[...]))
    for q in range(quantities):
        start = 2 * q * padded
        here = picked[start : start + basis] + picked[start + padded : start + padded + basis]
        value_ref[q : q + 1, :] = jnp.sum(here * weight_ref[...], axis=0, keepdims=True)
    half = LANES // 2
    lane = lax.broadcasted_iota(jnp.int32, (basis, LANES), 1)
    for start_lane in range(0, names_ref.shape[1], width):
        taken[...] = dot(split_ref[...], one_hot(elements, names_ref[:, start_lane : start_lane + width]))
        for part in range(width // LANES):
            slot = 2 * (start_lane // LANES + part)
            lanes = slice(part * LANES, (part + 1) * LANES)

            def of(q):
                start = 2 * q * padded
                return taken[start : start + basis, lanes] + taken[start + padded : start + padded + basis, lanes]

            for q in range(top):
                rows = slice(q * basis, (q + 1) * basis)
                upper = of(q)
                lower = of(q + top) if q + top < quantities else upper
                msg_ref[slot, rows, :] = jnp.where(lane < half, upper, pltpu.roll(lower, half, 1))
                msg_ref[slot + 1, rows, :] = jnp.where(lane < half, pltpu.roll(upper, half, 1), lower)


def local_kernel(padded, star_total, x_ref, matrix_ref, star_ref, face_ref, out_ref, terms):
    quantities, basis, _ = x_ref.shape
    total = matrix_ref.shape[0] // basis
    for q in range(quantities):
        high, low = split(pad_rows(x_ref[q], padded))
        terms[q] = dot(matrix_ref[...], jnp.concatenate([high, low, high], 0))
    for first, last in row_chunks(basis):
        sums = [jnp.zeros((last - first, x_ref.shape[2]), jnp.float32) for _ in range(quantities)]
        for n in range(total):
            ref, at = (star_ref, n) if n < star_total else (face_ref, n - star_total)
            for q in range(quantities):
                term = terms[q, n * basis + first : n * basis + last, :]
                if n >= star_total:
                    term = -term
                for p in range(quantities):
                    sums[p] = sums[p] + ref[at, p, q : q + 1, :] * term
        for p in range(quantities):
            out_ref[p, first:last, :] = sums[p]


def remote_kernel(padded, top, slots, *refs):
    x_ref, part_ref, split_ref, matrix_ref, face_ref, names_ref, live_ref = refs[:7]
    messages = refs[7 : 7 + slots]
    out_ref, wide, picked, terms = refs[7 + slots :]
    quantities, basis, width = x_ref.shape
    elements = split_ref.shape[1]
    faces = face_ref.shape[0]
    half = LANES // 2

    @pl.when(pl.program_id(0) == 0)
    def _():
        wide[:, :elements] = split_ref[...]
        lane = lax.broadcasted_iota(jnp.int32, (basis, LANES), 1)
        for pair in range(slots // 2):
            even, odd = messages[2 * pair], messages[2 * pair + 1]
            lanes = slice(elements + pair * LANES, elements + (pair + 1) * LANES)
            for q in range(quantities):
                if q < top:
                    rows = slice(q * basis, (q + 1) * basis)
                    value = jnp.where(lane < half, even[rows, :], pltpu.roll(odd[rows, :], half, 1))
                else:
                    rows = slice((q - top) * basis, (q - top + 1) * basis)
                    value = jnp.where(lane < half, pltpu.roll(even[rows, :], half, 1), odd[rows, :])
                high, low = split(pad_rows(value, padded))
                wide[2 * q * padded : (2 * q + 1) * padded, lanes] = high
                wide[(2 * q + 1) * padded : (2 * q + 2) * padded, lanes] = low

    for first_face in range(0, faces, 2):
        hot = jnp.concatenate(
            [one_hot(wide.shape[1], names_ref[f : f + 1, :]) for f in range(first_face, first_face + 2)], 1
        )
        picked[...] = dot(wide[...], hot).astype(jnp.bfloat16)
        for q in range(quantities):
            start = 2 * q * padded
            for f in range(first_face, first_face + 2):
                lanes = slice((f - first_face) * width, (f - first_face + 1) * width)
                both = picked[start : start + 2 * padded, lanes]
                terms[q, f * basis : (f + 1) * basis, :] = dot(
                    matrix_ref[f], jnp.concatenate([both, both[:padded]], 0)
                )
    live = live_ref[...] > 0.5
    for first, last in row_chunks(basis):
        sums = [jnp.zeros((last - first, width), jnp.float32) for _ in range(quantities)]
        for f in range(faces):
            for q in range(quantities):
                term = terms[q, f * basis + first : f * basis + last, :]
                for p in range(quantities):
                    sums[p] = sums[p] + face_ref[f, p, q : q + 1, :] * term
        for p in range(quantities):
            field = x_ref[p, first:last, :]
            out_ref[p, first:last, :] = jnp.where(live, field + (part_ref[p, first:last, :] - sums[p]), field)


def halo_ways(slot_number):
    if slot_number < PEER_REACH:
        return "dom", slot_number + 1
    if slot_number < 2 * PEER_REACH:
        return "dom", PEER_REACH - 1 - slot_number
    return "grp", 1 if slot_number == 2 * PEER_REACH else -1


def send(value, slot_number):
    axis, by = halo_ways(slot_number)
    count = lax.axis_size(axis)
    if axis == "dom":
        pairs = [(i, (i + by) % count) for i in range(count)]
    else:
        pairs = [(i, i + by) for i in range(count) if 0 <= i + by < count]
    return lax.ppermute(value, axis, pairs)


def per_device(
    element_state,
    stiffness,
    flux_local,
    flux_remote,
    star_matrix,
    face_local,
    face_remote,
    energy_weight,
    face_neighbour,
    element_count,
    send_count,
    send_element,
    receiver_element,
    receiver_slot,
    receiver_weight,
):
    basis, quantities, elements = element_state.shape
    slots, capacity = send_element.shape[1:]
    receivers = receiver_slot.shape[0]
    dimensions, faces = stiffness.shape[0], flux_local.shape[0]
    group_size = lax.axis_size("dom")
    padded = round_up(basis, 16)
    top = (quantities + 1) // 2
    f32, bf16 = jnp.float32, jnp.bfloat16
    width = LANES
    blocks = elements // width

    local_matrix = stacked_matrix(jnp.concatenate([stiffness, flux_local], 0))
    local_matrix = local_matrix.reshape(-1, local_matrix.shape[2])
    remote_matrix = stacked_matrix(flux_remote)
    slot_live = jnp.arange(capacity)[None, :] < send_count[0][:, None]
    names = jnp.where(slot_live, send_element[0], -1).reshape(1, -1)
    rec_names = jnp.pad(receiver_element[None, :], ((0, 0), (0, LANES - receivers)), constant_values=-1)
    rec_weight = jnp.pad(receiver_weight, ((0, 0), (0, LANES - receivers)))
    live = (jnp.arange(elements)[None, :] < element_count[0]).astype(f32)
    gains = energy_weight * live
    fields = jnp.transpose(element_state, (1, 0, 2))

    pack = pl.pallas_call(
        functools.partial(pack_kernel, padded, top),
        out_shape=(
            jax.ShapeDtypeStruct((slots, top * basis, LANES), f32),
            jax.ShapeDtypeStruct((2 * quantities * padded, elements), bf16),
            jax.ShapeDtypeStruct((quantities, LANES), f32),
            jax.ShapeDtypeStruct((1, elements), f32),
        ),
        scratch_shapes=[pltpu.VMEM((2 * quantities * padded, 2 * LANES), f32)],
        compiler_params=pltpu.CompilerParams(vmem_limit_bytes=40 << 20),
        cost_estimate=pl.CostEstimate(flops=2_000_000_000, bytes_accessed=5_000_000, transcendentals=0),
        name="pack",
    )
    block = pl.BlockSpec((quantities, basis, width), lambda i: (0, 0, i))

    def whole(array):
        rank = len(array.shape)
        return pl.BlockSpec(array.shape, lambda i: (0,) * rank)

    def coefficients(array):
        return pl.BlockSpec(array.shape[:3] + (width,), lambda i: (0, 0, 0, i))

    state = jax.ShapeDtypeStruct((quantities, basis, elements), f32)
    local = pl.pallas_call(
        functools.partial(local_kernel, padded, dimensions),
        out_shape=state,
        grid=(blocks,),
        in_specs=[block, whole(local_matrix), coefficients(star_matrix), coefficients(face_local)],
        out_specs=block,
        scratch_shapes=[pltpu.VMEM((quantities, local_matrix.shape[0], width), f32)],
        compiler_params=pltpu.CompilerParams(vmem_limit_bytes=40 << 20),
        cost_estimate=pl.CostEstimate(flops=8_000_000_000, bytes_accessed=6_000_000, transcendentals=0),
        name="local",
    )
    split_shape = jax.ShapeDtypeStruct((2 * quantities * padded, elements), bf16)
    message = jax.ShapeDtypeStruct((top * basis, LANES), f32)
    remote = pl.pallas_call(
        functools.partial(remote_kernel, padded, top, slots),
        out_shape=state,
        grid=(blocks,),
        in_specs=[
            block,
            block,
            whole(split_shape),
            whole(remote_matrix),
            coefficients(face_remote),
            pl.BlockSpec((faces, width), lambda i: (0, i)),
            pl.BlockSpec((1, width), lambda i: (0, i)),
        ]
        + [whole(message)] * slots,
        out_specs=block,
        scratch_shapes=[
            pltpu.VMEM((2 * quantities * padded, elements + slots * capacity), bf16),
            pltpu.VMEM((2 * quantities * padded, 2 * width), bf16),
            pltpu.VMEM((quantities, faces * basis, width), f32),
        ],
        compiler_params=pltpu.CompilerParams(vmem_limit_bytes=40 << 20),
        cost_estimate=pl.CostEstimate(flops=8_000_000_000, bytes_accessed=6_000_000, transcendentals=0),
        name="remote",
    )

    values = []
    energies = []
    messages, halves, _, _ = pack(fields, names, rec_weight, rec_names, gains)
    for time_step in range(TIME_STEPS):
        arrived = [send(messages[slot], slot) for slot in range(slots)]
        partial = local(fields, local_matrix, star_matrix, face_local)
        fields = remote(fields, partial, halves, remote_matrix, face_remote, face_neighbour, live, *arrived)
        messages, halves, value, energy = pack(fields, names, rec_weight, rec_names, gains)
        values.append(value)
        energies.append(energy)
    own_energy = 0.5 * jnp.sum(jnp.concatenate(energies, 0), axis=1)
    slot_row = receiver_slot.astype(f32)[None, :]
    table = jnp.concatenate(
        [
            jnp.concatenate(values, 0)[:, :receivers],
            slot_row,
            jnp.broadcast_to(own_energy[:, None], (TIME_STEPS, receivers)),
        ],
        0,
    )
    everyone = lax.all_gather(table, "dom", axis=1, tiled=True)
    count = TIME_STEPS * quantities
    mine = (lax.axis_index("dom") * receivers + jnp.arange(receivers)).astype(f32)
    matches = (everyone[count][:, None] == mine[None, :]).astype(f32)
    traces = jnp.dot(everyone[:count], matches, precision=lax.Precision.HIGHEST, preferred_element_type=f32)
    denominator = float(group_size * elements * basis * quantities)
    by_partition = everyone[count + 1 :].reshape(TIME_STEPS, group_size, receivers)[:, :, 0]
    energy = jnp.sum(by_partition, axis=1) / denominator
    return (
        jnp.transpose(fields, (1, 0, 2)),
        energy[None, :],
        traces.reshape(TIME_STEPS, quantities, receivers),
    )


def solution(mesh):
    both = ("grp", "dom")
    return jax.shard_map(
        per_device,
        mesh=mesh,
        in_specs=(
            P(None, None, both),
            P(),
            P(),
            P(),
            P(None, None, None, both),
            P(None, None, None, both),
            P(None, None, None, both),
            P(None, both),
            P(None, both),
            P(both),
            P(both, None),
            P(both, None, None),
            P(both),
            P(both),
            P(None, both),
        ),
        out_specs=(P(None, None, both), P("grp", None), P(None, None, both)),
        check_vma=False,
    )
```

```python
import functools

import jax
import jax.numpy as jnp
from jax import lax
from jax.experimental import pallas as pl
from jax.experimental.pallas import tpu as pltpu
from jax.sharding import PartitionSpec as P

PEER_REACH = 3
TIME_STEPS = 3
LANES = 128


def one_hot(rows, names):
    place = lax.broadcasted_iota(jnp.int32, (rows, names.shape[1]), 0)
    return jnp.where(place == names, 1.0, 0.0).astype(jnp.bfloat16)


def dot(a, b):
    return jnp.dot(a, b, preferred_element_type=jnp.float32)


def stacked_matrix(matrices):
    high = lax.reduce_precision(matrices, 8, 7)
    low = (matrices - high).astype(jnp.bfloat16)
    high = high.astype(jnp.bfloat16)
    return jnp.concatenate([high, high, low, low], 2)


def row_chunks(rows):
    middle = min(rows, 32)
    return [(0, middle), (middle, rows)] if middle < rows else [(0, rows)]


def split_rows(field):
    high = field.astype(jnp.bfloat16).astype(jnp.float32)
    return jnp.concatenate([high, field - high], 0).astype(jnp.bfloat16)


def pack_kernel(top, x_ref, names_ref, weight_ref, rec_ref, gains_ref, msg_ref, split_ref, value_ref, energy_ref, taken):
    quantities, basis, elements = x_ref.shape
    width = 2 * LANES
    total = jnp.zeros((1, elements), jnp.float32)
    for q in range(quantities):
        field = x_ref[q]
        total = total + gains_ref[q : q + 1, :] * jnp.sum(field * field, axis=0, keepdims=True)
        split_ref[2 * q * basis : 2 * (q + 1) * basis, :] = split_rows(field)
    energy_ref[...] = total
    picked = dot(split_ref[...], one_hot(elements, rec_ref[...]))
    for q in range(quantities):
        start = 2 * q * basis
        here = picked[start : start + basis] + picked[start + basis : start + 2 * basis]
        value_ref[q : q + 1, :] = jnp.sum(here * weight_ref[...], axis=0, keepdims=True)
    half = LANES // 2
    lane = lax.broadcasted_iota(jnp.int32, (basis, LANES), 1)
    for start_lane in range(0, names_ref.shape[1], width):
        taken[...] = dot(split_ref[...], one_hot(elements, names_ref[:, start_lane : start_lane + width]))
        for part in range(width // LANES):
            slot = 2 * (start_lane // LANES + part)
            lanes = slice(part * LANES, (part + 1) * LANES)

            def of(q):
                start = 2 * q * basis
                return taken[start : start + basis, lanes] + taken[start + basis : start + 2 * basis, lanes]

            for q in range(top):
                rows = slice(q * basis, (q + 1) * basis)
                upper = of(q)
                lower = of(q + top) if q + top < quantities else upper
                msg_ref[slot, rows, :] = jnp.where(lane < half, upper, pltpu.roll(lower, half, 1))
                msg_ref[slot + 1, rows, :] = jnp.where(lane < half, pltpu.roll(upper, half, 1), lower)


def halo_ways(slot_number):
    if slot_number < PEER_REACH:
        return "dom", slot_number + 1
    if slot_number < 2 * PEER_REACH:
        return "dom", PEER_REACH - 1 - slot_number
    return "grp", 1 if slot_number == 2 * PEER_REACH else -1


def peer(axis, by):
    place = lax.axis_index(axis)
    count = lax.axis_size(axis)
    if axis == "dom":
        return {axis: lax.rem(place + by + count, count)}, None
    other = place + by
    return {axis: jnp.clip(other, 0, count - 1)}, (other >= 0) & (other < count)


def guarded(condition, action):
    if condition is None:
        action()
    else:
        pl.when(condition)(action)


def local_kernel(x_ref, matrix_ref, star_ref, face_ref, msg_ref, out_ref, halo_ref, held, terms, send_sem, recv_sem):
    quantities, basis, elements = x_ref.shape
    slots = msg_ref.shape[0]
    star_total, face_total = star_ref.shape[2], face_ref.shape[2]
    barrier = pltpu.get_barrier_semaphore()
    ways = [halo_ways(slot) for slot in range(slots)]
    for way in ways:
        device, there = peer(*way)
        guarded(
            there,
            lambda: pl.semaphore_signal(barrier, inc=1, device_id=device, device_id_type=pl.DeviceIdType.MESH),
        )
    greeted = 0
    for way in ways:
        _, there = peer(*way)
        greeted = greeted + (1 if there is None else there.astype(jnp.int32))
    pl.semaphore_wait(barrier, greeted)

    def copy(slot):
        device, there = peer(*ways[slot])
        return (
            pltpu.make_async_remote_copy(
                src_ref=msg_ref.at[slot],
                dst_ref=held.at[slot],
                send_sem=send_sem.at[slot],
                recv_sem=recv_sem.at[slot],
                device_id=device,
                device_id_type=pl.DeviceIdType.MESH,
            ),
            there,
        )

    for slot in range(slots):
        sent, there = copy(slot)
        guarded(there, sent.start)

    def one_block(number, carry):
        lanes = pl.ds(pl.multiple_of(number * LANES, LANES), LANES)

        for q in range(quantities):
            both = split_rows(x_ref[q, :, lanes])
            terms[q] = dot(matrix_ref[...], jnp.concatenate([both, both], 0))
        for first, last in row_chunks(basis):

            def one_quantity(q, sums):
                for n in range(star_total + face_total):
                    ref, at = (star_ref, n) if n < star_total else (face_ref, n - star_total)
                    term = terms[q, n * basis + first : n * basis + last, :]
                    sums = sums + ref[:, q, at : at + 1, lanes] * term[None]
                return sums

            start = jnp.zeros((quantities, last - first, LANES), jnp.float32)
            out_ref[:, first:last, lanes] = lax.fori_loop(0, quantities, one_quantity, start)
        return carry

    lax.fori_loop(0, elements // LANES, one_block, 0)
    for slot in range(slots):
        sent, there = copy(slot)
        guarded(there, sent.wait_send)
        axis, by = ways[slot]
        _, came = peer(axis, -by)

        def take(sent=sent, slot=slot):
            sent.wait_recv()
            halo_ref[slot] = held[slot]

        guarded(came, take)
        if came is not None:

            @pl.when(jnp.logical_not(came))
            def _(slot=slot):
                halo_ref[slot] = jnp.zeros(held.shape[1:], jnp.float32)


def remote_kernel(top, x_ref, part_ref, split_ref, matrix_ref, face_ref, names_ref, live_ref, halo_ref, out_ref, wide, *scratch):
    quantities, basis, width = x_ref.shape
    elements = split_ref.shape[1]
    faces = face_ref.shape[2]
    slots = halo_ref.shape[0]
    half = LANES // 2

    @pl.when(pl.program_id(0) == 0)
    def _():
        wide[:, :elements] = split_ref[...]
        lane = lax.broadcasted_iota(jnp.int32, (basis, LANES), 1)
        for pair in range(slots // 2):
            lanes = slice(elements + pair * LANES, elements + (pair + 1) * LANES)
            for q in range(quantities):
                at = q if q < top else q - top
                rows = slice(at * basis, (at + 1) * basis)
                even, odd = halo_ref[2 * pair, rows, :], halo_ref[2 * pair + 1, rows, :]
                if q < top:
                    value = jnp.where(lane < half, even, pltpu.roll(odd, half, 1))
                else:
                    value = jnp.where(lane < half, pltpu.roll(even, half, 1), odd)
                wide[2 * q * basis : 2 * (q + 1) * basis, lanes] = split_rows(value)

    pairs = faces // 2
    picked, terms = scratch[:pairs], scratch[pairs : 2 * pairs]
    for pair in range(pairs):
        hot = jnp.concatenate(
            [one_hot(wide.shape[1], names_ref[f : f + 1, :]) for f in (2 * pair, 2 * pair + 1)], 1
        )
        picked[pair][...] = dot(wide[...], hot).astype(jnp.bfloat16)
        for q in range(quantities):
            for f in range(2):
                both = picked[pair][2 * q * basis : 2 * (q + 1) * basis, f * width : (f + 1) * width]
                terms[pair][q, f * basis : (f + 1) * basis, :] = dot(
                    matrix_ref[2 * pair + f], jnp.concatenate([both, both], 0)
                )
    live = live_ref[...] > 0.5
    for first, last in row_chunks(basis):
        sums = [jnp.zeros((last - first, width), jnp.float32) for _ in range(quantities)]
        for f in range(faces):
            for q in range(quantities):
                term = terms[f // 2][q, f % 2 * basis + first : f % 2 * basis + last, :]
                for p in range(quantities):
                    sums[p] = sums[p] + face_ref[p, q, f : f + 1, :] * term
        for p in range(quantities):
            field = x_ref[p, first:last, :]
            out_ref[p, first:last, :] = jnp.where(live, field + (part_ref[p, first:last, :] - sums[p]), field)


def gather_kernel(axis, table_ref, all_ref, held, send_sem, recv_sem):
    count = lax.axis_size(axis)
    me = lax.axis_index(axis)
    barrier = pltpu.get_barrier_semaphore()

    def other(step):
        return lax.rem(me + step, count)

    def greet(step, carry):
        pl.semaphore_signal(
            barrier, inc=1, device_id={axis: other(step)}, device_id_type=pl.DeviceIdType.MESH
        )
        return carry

    lax.fori_loop(1, count, greet, 0)
    pl.semaphore_wait(barrier, count - 1)

    def copy(step, slot):
        return pltpu.make_async_remote_copy(
            src_ref=table_ref,
            dst_ref=held.at[slot],
            send_sem=send_sem.at[step],
            recv_sem=recv_sem.at[slot],
            device_id={axis: other(step)},
            device_id_type=pl.DeviceIdType.MESH,
        )

    def start(step, carry):
        copy(step, me).start()
        return carry

    lax.fori_loop(1, count, start, 0)

    def finish(step, carry):
        copy(step, me).wait_send()
        source = other(step)
        copy(step, source).wait_recv()
        all_ref[source] = held[source]
        return carry

    lax.fori_loop(1, count, finish, 0)
    all_ref[me] = table_ref[...]


def per_device(
    element_state,
    stiffness,
    flux_local,
    flux_remote,
    star_matrix,
    face_local,
    face_remote,
    energy_weight,
    face_neighbour,
    element_count,
    send_count,
    send_element,
    receiver_element,
    receiver_slot,
    receiver_weight,
):
    basis, quantities, elements = element_state.shape
    slots, capacity = send_element.shape[1:]
    receivers = receiver_slot.shape[0]
    dimensions, faces = stiffness.shape[0], flux_local.shape[0]
    group_size = lax.axis_size("dom")
    top = (quantities + 1) // 2
    f32, bf16 = jnp.float32, jnp.bfloat16
    width = LANES
    blocks = elements // width

    local_matrix = stacked_matrix(jnp.concatenate([stiffness, -flux_local], 0))
    local_matrix = local_matrix.reshape(-1, local_matrix.shape[2])
    remote_matrix = stacked_matrix(flux_remote)
    slot_live = jnp.arange(capacity)[None, :] < send_count[0][:, None]
    names = jnp.where(slot_live, send_element[0], -1).reshape(1, -1)
    rec_names = jnp.pad(receiver_element[None, :], ((0, 0), (0, LANES - receivers)), constant_values=-1)
    rec_weight = jnp.pad(receiver_weight, ((0, 0), (0, LANES - receivers)))
    live = (jnp.arange(elements)[None, :] < element_count[0]).astype(f32)
    gains = energy_weight * live
    fields = jnp.transpose(element_state, (1, 0, 2))
    stars = jnp.transpose(star_matrix, (1, 2, 0, 3))
    near = jnp.transpose(face_local, (1, 2, 0, 3))
    far = jnp.transpose(face_remote, (1, 2, 0, 3))

    pack = pl.pallas_call(
        functools.partial(pack_kernel, top),
        out_shape=(
            jax.ShapeDtypeStruct((slots, top * basis, LANES), f32),
            jax.ShapeDtypeStruct((2 * quantities * basis, elements), bf16),
            jax.ShapeDtypeStruct((quantities, LANES), f32),
            jax.ShapeDtypeStruct((1, elements), f32),
        ),
        scratch_shapes=[pltpu.VMEM((2 * quantities * basis, 2 * LANES), f32)],
        compiler_params=pltpu.CompilerParams(vmem_limit_bytes=40 << 20),
        cost_estimate=pl.CostEstimate(flops=2_000_000_000, bytes_accessed=5_000_000, transcendentals=0),
        name="pack",
    )
    block = pl.BlockSpec((quantities, basis, width), lambda i: (0, 0, i))

    def whole(array):
        rank = len(array.shape)
        return pl.BlockSpec(array.shape, lambda i: (0,) * rank)

    def coefficients(array):
        return pl.BlockSpec(array.shape[:3] + (width,), lambda i: (0, 0, 0, i))

    state = jax.ShapeDtypeStruct((quantities, basis, elements), f32)
    mail = jax.ShapeDtypeStruct((slots, top * basis, LANES), f32)
    in_vmem = pl.BlockSpec(memory_space=pltpu.VMEM)
    local = pl.pallas_call(
        local_kernel,
        out_shape=(state, mail),
        in_specs=[in_vmem] * 5,
        out_specs=(in_vmem, in_vmem),
        scratch_shapes=[
            pltpu.VMEM(mail.shape, f32),
            pltpu.VMEM((quantities, local_matrix.shape[0], width), f32),
            pltpu.SemaphoreType.DMA((slots,)),
            pltpu.SemaphoreType.DMA((slots,)),
        ],
        compiler_params=pltpu.CompilerParams(
            vmem_limit_bytes=40 << 20, collective_id=0, has_side_effects=True
        ),
        name="local",
    )
    split_shape = jax.ShapeDtypeStruct((2 * quantities * basis, elements), bf16)
    remote = pl.pallas_call(
        functools.partial(remote_kernel, top),
        out_shape=state,
        grid=(blocks,),
        in_specs=[
            block,
            block,
            whole(split_shape),
            whole(remote_matrix),
            coefficients(far),
            pl.BlockSpec((faces, width), lambda i: (0, i)),
            pl.BlockSpec((1, width), lambda i: (0, i)),
            whole(mail),
        ],
        out_specs=block,
        scratch_shapes=[
            pltpu.VMEM((2 * quantities * basis, elements + slots * capacity), bf16),
        ]
        + [pltpu.VMEM((2 * quantities * basis, 2 * width), bf16)] * (faces // 2)
        + [pltpu.VMEM((quantities, 2 * basis, width), f32)] * (faces // 2),
        compiler_params=pltpu.CompilerParams(vmem_limit_bytes=40 << 20),
        cost_estimate=pl.CostEstimate(flops=8_000_000_000, bytes_accessed=6_000_000, transcendentals=0),
        name="remote",
    )

    values = []
    energies = []
    messages, halves, _, _ = pack(fields, names, rec_weight, rec_names, gains)
    for time_step in range(TIME_STEPS):
        partial, halo = local(fields, local_matrix, stars, near, messages)
        fields = remote(fields, partial, halves, remote_matrix, far, face_neighbour, live, halo)
        messages, halves, value, energy = pack(fields, names, rec_weight, rec_names, gains)
        values.append(value)
        energies.append(energy)
    own_energy = 0.5 * jnp.sum(jnp.concatenate(energies, 0), axis=1)
    slot_row = receiver_slot.astype(f32)[None, :]
    table = jnp.concatenate(
        [
            jnp.concatenate(values, 0)[:, :receivers],
            slot_row,
            jnp.broadcast_to(own_energy[:, None], (TIME_STEPS, receivers)),
        ],
        0,
    )
    rows = (table.shape[0] + 7) // 8 * 8
    table = jnp.pad(table, ((0, rows - table.shape[0]), (0, LANES - receivers)))
    everyone = pl.pallas_call(
        functools.partial(gather_kernel, "dom"),
        out_shape=jax.ShapeDtypeStruct((group_size, rows, LANES), f32),
        in_specs=[in_vmem],
        out_specs=in_vmem,
        scratch_shapes=[
            pltpu.VMEM((group_size, rows, LANES), f32),
            pltpu.SemaphoreType.DMA((group_size,)),
            pltpu.SemaphoreType.DMA((group_size,)),
        ],
        compiler_params=pltpu.CompilerParams(collective_id=1, has_side_effects=True),
        name="gather",
    )(table)[:, :, :receivers]
    count = TIME_STEPS * quantities
    mine = (lax.axis_index("dom") * receivers + jnp.arange(receivers)).astype(f32)
    matches = (everyone[:, count, :, None] == mine).astype(f32)
    traces = jnp.einsum(
        "dkr,drs->ks", everyone[:, :count], matches, precision=lax.Precision.HIGHEST, preferred_element_type=f32
    )
    denominator = float(group_size * elements * basis * quantities)
    energy = jnp.sum(everyone[:, count + 1 : count + 1 + TIME_STEPS, 0], axis=0) / denominator
    return (
        jnp.transpose(fields, (1, 0, 2)),
        energy[None, :],
        traces.reshape(TIME_STEPS, quantities, receivers),
    )


def solution(mesh):
    both = ("grp", "dom")
    return jax.shard_map(
        per_device,
        mesh=mesh,
        in_specs=(
            P(None, None, both),
            P(),
            P(),
            P(),
            P(None, None, None, both),
            P(None, None, None, both),
            P(None, None, None, both),
            P(None, both),
            P(None, both),
            P(both),
            P(both, None),
            P(both, None, None),
            P(both),
            P(both),
            P(None, both),
        ),
        out_specs=(P(None, None, both), P("grp", None), P(None, None, both)),
        check_vma=False,
    )
```
